1024 devices in a mesh: dp: 32 (over z_hi, y, core), expert: 32 (over z_lo, x).
Axes of the slice: x: 4, y: 4, z: 32 (z_hi: 4, z_lo: 8; z = z_hi * 8 + z_lo), core: 2. Of those that a mesh axis runs over, the one named last changes fastest.
Arguments:
- hidden: bfloat16 [262144, 768], P(('dp', 'expert')), may hold values from -6 to 6
- w_down: bfloat16 [32, 768, 2048], P('expert', 'dp'), may hold values from -0.21875 to 0.21875
- expert_ids: int32 [32768, 4], P(('dp', 'expert')), may hold values from 0 to 31, all different within a row; in each aligned block of 32 rows (0 to 31, 32 to 63, ...) at most 8 rows name the same one
- gates: float32 [32768, 4], P(('dp', 'expert')), may hold values from 0.05 to 1
- cotangent: bfloat16 [32768, 2048], P(('dp', 'expert')), may hold values from -6 to 6
Outputs:
- mixed: bfloat16 [32768, 2048], P(('dp', 'expert'))
- gate_grads: float32 [32768, 4], P(('dp', 'expert'))
- hidden_grads: bfloat16 [262144, 768], P(('dp', 'expert'))
- weight_grads: bfloat16 [32, 768, 2048], P('expert', 'dp')
The draws below stay inside these ranges and needn't reach their ends.
Inputs may be any that keep to these rules, and one draw needn't show every extreme that they name: `expert_ids`: each row names 4 different experts. Among the rows of one device no expert is named more than 8 times, a bound that some block reaches.
All inputs are finite; a program needn't handle non-finite values.
Results may differ from the reference program's by a relative error of at most 0.015.
Values may be sent and summed in bfloat16 or wider, within the bound.
No kernel may reach another device: no remote copies, remote signals or barrier semaphores. Data moves between devices by JAX's collectives and lax.ppermute only.
A program may use at most 32 MiB of HBM per device.

```python
import math
import jax
import jax.numpy as jnp
import numpy as np
from jax import lax

D = 2048
F = 768
TOPK = 4
TOK_DEV = 32
CAP = 8
RECV = 256
EXPERTS = 32
TOKENS = 32768
N_DP = 32
N_EXPERT = 32


def level_of(rng, dims, shards, smallest, high):
    loudness, own = 1.0, jax.random.fold_in(rng, 6)
    for dim, shards_of in shards:
        heights = jnp.exp(jax.random.uniform(jax.random.fold_in(own, dim), (shards_of,), jnp.float32, smallest / len(shards), high / len(shards)))
        loudness = loudness * jnp.repeat(heights, dims[dim] // shards_of).reshape([-1 if axis == dim else 1 for axis in range(len(dims))])
    return loudness


def assign_block(stream_key, own, number, rows, amount, top, reach, slope):
    ranking = jax.random.permutation(stream_key, amount)
    crowded, common = shares(amount, rows * top, reach, slope, True), shares(amount, rows * top, reach, slope, False)
    places = jnp.arange(amount)

    def named(lengths, offset_by):
        used = int((lengths > 0).sum())
        fixed = max(1, used // 4)
        shifted = fixed + (places - fixed + offset_by * (used - fixed)) % max(1, amount - fixed)
        return jnp.zeros((amount,), jnp.int32).at[ranking[jnp.where(places < fixed, places, shifted)]].set(jnp.asarray(lengths, jnp.int32))

    lengths = jnp.where(number % 4 == 0, named(crowded, number // 4), named(common, number - number // 4 - 1))
    mixed = jax.random.permutation(jax.random.fold_in(own, 3), amount)
    giver, receiver = mixed[0:amount // 2 * 2:2], mixed[1:amount // 2 * 2:2]
    room = jnp.minimum(lengths[giver] - 1, reach - lengths[receiver]) // 2
    room = jnp.where((giver == ranking[0]) | (receiver == ranking[0]) | (lengths[receiver] == 0), 0, jnp.maximum(room, 0))
    shifted = jax.random.randint(jax.random.fold_in(own, 4), (amount // 2,), 0, 1 << 20) % (room + 1)
    lengths = lengths.at[giver].add(-shifted).at[receiver].add(shifted)
    labels = jnp.searchsorted(jnp.cumsum(lengths), jnp.arange(rows * top), side="right").astype(jnp.int32)
    table = labels.reshape(top, rows).T
    table = table[jax.random.permutation(jax.random.fold_in(own, 1), rows)]
    offset_by = jax.random.randint(jax.random.fold_in(own, 2), (rows, 1), 0, top)
    return jnp.take_along_axis(table, (jnp.arange(top)[None, :] + offset_by) % top, axis=1)


def shares(amount, total, bound, slope, full):
    portions = [(1 << 20) // math.isqrt(grade ** slope) + 1 for grade in range(1, amount + 1)]
    largest = bound if full else min(bound, max(-(-total // amount), total * portions[0] // sum(portions)))
    least = 1 if total - largest >= amount - 1 else 0
    holding, spare = [largest] + [least] * (amount - 1), total - largest - least * (amount - 1)
    while spare > 0:
        movable = [i for i in range(1, amount) if holding[i] < largest] or [i for i in range(1, amount) if holding[i] < bound]
        mass, left = sum([portions[i] for i in movable]), spare
        for i in movable:
            extra = min(bound - holding[i], max(1, left * portions[i] // mass), spare)
            holding[i] = holding[i] + extra
            spare = spare - extra
    return np.array(holding)


def bell_draw(own_key, shape, deviation, limit, cuts=(), kind=jnp.bfloat16):
    factor_of = level_of(own_key, shape, cuts, -0.22, 0.18) if cuts else 1.0
    result = jax.random.normal(own_key, shape, jnp.float32) * deviation * factor_of
    return jnp.minimum(jnp.maximum(result, -limit), limit).astype(kind)


def setup_inputs(seed: int = 0) -> dict:
    splits = jax.random.split(jax.random.key(seed), 6)
    hidden = bell_draw(splits[0], (N_DP * N_EXPERT * RECV, F), 1.0, 6.0, ((0, 1024),))
    w_down = bell_draw(splits[1], (EXPERTS, F, D), F ** -0.5, 0.21875, ((0, 32), (1, 32)))
    expert_ids_keys = jax.random.split(jax.random.fold_in(splits[2], 1), TOKENS // TOK_DEV)
    expert_ids_turns = jax.random.permutation(jax.random.fold_in(splits[2], 3), TOKENS // TOK_DEV)
    expert_ids = jax.vmap(lambda own, number: assign_block(jax.random.fold_in(splits[2], 2), own, number, TOK_DEV, N_EXPERT, TOPK, CAP, 2))(expert_ids_keys, expert_ids_turns).reshape((TOKENS, TOPK))
    gates = jnp.clip(jnp.exp(math.log(1.0) - 2.9957323 * jax.random.uniform(splits[3], (TOKENS, TOPK), jnp.float32) ** level_of(splits[3], (TOKENS, TOPK), ((0, 1024),), -0.2, 0.2)), 0.05, 1.0)
    cotangent = bell_draw(splits[4], (TOKENS, D), 1.0, 6.0, ((0, 1024),))
    return {"hidden": hidden, "w_down": w_down, "expert_ids": expert_ids, "gates": gates, "cotangent": cotangent}


def positions(flat_ids):
    choose = (flat_ids[:, None] == jnp.arange(N_EXPERT, dtype=jnp.int32)[None, :]).astype(jnp.int32)
    earlier = jnp.cumsum(choose, axis=0) - choose
    return jnp.sum(earlier * choose, axis=1).astype(jnp.int32)


def reference(hidden, w_down, expert_ids, gates, cotangent):
    h_all = hidden.reshape(N_DP, N_EXPERT, N_EXPERT, CAP, F)
    id_all = expert_ids.reshape(N_DP, N_EXPERT, TOK_DEV, TOPK)
    gate_all = gates.reshape(N_DP, N_EXPERT, TOK_DEV, TOPK)
    cot_all = cotangent.reshape(N_DP, N_EXPERT, TOK_DEV, D)
    weight32 = w_down.astype(jnp.float32)
    senders = jnp.arange(N_EXPERT, dtype=jnp.int32)[:, None]
    highest = lax.Precision.HIGHEST

    def one_row(total, pieces):
        h_row, id_row, gate_row, cot_row = pieces
        h32 = h_row.astype(jnp.float32)
        outputs = jnp.einsum("ebcf,efd->ebcd", h32, weight32, precision=highest).astype(jnp.bfloat16)
        flat_ids = id_row.reshape(N_EXPERT, TOK_DEV * TOPK)
        position = jax.vmap(positions)(flat_ids)
        sender_ids = jnp.broadcast_to(senders, flat_ids.shape)
        picked = outputs[flat_ids, sender_ids, position].astype(jnp.float32).reshape(N_EXPERT, TOK_DEV, TOPK, D)
        cot32 = cot_row.astype(jnp.float32)
        mixed = jnp.sum(gate_row[..., None] * picked, axis=2).astype(jnp.bfloat16)
        gate_grads = jnp.sum(picked * cot32[:, :, None, :], axis=3)
        routed = (gate_row[..., None] * cot32[:, :, None, :]).astype(jnp.bfloat16).reshape(N_EXPERT, TOK_DEV * TOPK, D)
        grads_in = jnp.zeros((N_EXPERT, N_EXPERT, CAP, D), jnp.bfloat16).at[flat_ids, sender_ids, position].set(routed)
        grads32 = grads_in.astype(jnp.float32)
        hidden_grads = jnp.einsum("ebcd,efd->ebcf", grads32, weight32, precision=highest).astype(jnp.bfloat16)
        partial_sum = jnp.einsum("ebcf,ebcd->efd", h32, grads32, precision=highest).astype(jnp.bfloat16)
        partial_sum = lax.optimization_barrier(partial_sum)
        return total + partial_sum.astype(jnp.float32), (mixed, gate_grads, hidden_grads)

    start_total = jnp.zeros((N_EXPERT, F, D), jnp.float32)
    total, stacked = lax.scan(one_row, start_total, (h_all, id_all, gate_all, cot_all))
    mixed, gate_grads, hidden_grads = stacked
    return (mixed.reshape(N_DP * N_EXPERT * TOK_DEV, D), gate_grads.reshape(N_DP * N_EXPERT * TOK_DEV, TOPK), hidden_grads.reshape(N_DP * N_EXPERT * N_EXPERT * CAP, F), total.astype(jnp.bfloat16))
```

```python
import jax
import jax.numpy as jnp
from jax import lax
from jax.sharding import Mesh
from jax.sharding import PartitionSpec as P


ZH, Y, CORE, HALF, GRP = "zh", "y", "core", "half", "grp"
DP = (ZH, Y, CORE)
ALL = (ZH, Y, CORE, HALF, GRP)
N_ZH, N_Y, N_CORE, N_HALF = 4, 4, 2, 2
RING = 4
RIGHT = [(i, (i + 1) % RING) for i in range(RING)]
LEFT = [(i, (i - 1) % RING) for i in range(RING)]
SWAP = [(0, 1), (1, 0)]
F32, BF16 = jnp.float32, jnp.bfloat16


def dot(a, b, dims):
    return lax.dot_general(a, b, (dims, ((), ())), preferred_element_type=F32)


def exchange(rows, axis):
    return lax.all_to_all(rows, axis, split_axis=0, concat_axis=0, tiled=True)


def slots_of(ids, gates, cotangent, first_expert, experts, capacity):
    tokens, top = ids.shape
    line = jnp.arange(experts * capacity, dtype=jnp.int32)[:, None]
    expert = first_expert + line // capacity
    same = [expert == ids[:, k][None, :] for k in range(top)]
    named = same[0]
    gate = jnp.where(same[0], gates[:, 0][None, :], 0.0)
    for k in range(1, top):
        named = named | same[k]
        gate = jnp.where(same[k], gates[:, k][None, :], gate)
    order = jnp.arange(tokens, dtype=jnp.int32)
    before = (order[:, None] < order[None, :]).astype(BF16)
    earlier = dot(named.astype(BF16), before, ((1,), (0,)))
    fills = named & (earlier == (line % capacity).astype(F32))
    slot_gate = jnp.sum(jnp.where(fills, gate, 0.0), axis=1, keepdims=True)
    rows = dot(fills.astype(BF16), cotangent, ((1,), (0,)))
    return fills, same, slot_gate, rows


def combine(returned, fills, same, slot_gate, rows):
    weight = jnp.where(fills, slot_gate, 0.0)
    high = lax.reduce_precision(weight, 8, 7)
    low = (weight - high).astype(BF16)
    mixed = dot(high.astype(BF16), returned, ((0,), (0,))) + dot(low, returned, ((0,), (0,)))
    inner = jnp.sum(returned.astype(F32) * rows.astype(F32), axis=1, keepdims=True)
    spread = jnp.where(fills, inner, 0.0)
    grads = jnp.stack([jnp.sum(jnp.where(s, spread, 0.0), axis=0) for s in same], axis=0)
    return mixed, grads


def gather_ring(own, axis):
    here = lax.axis_index(axis)
    half = own.shape[-1] // 2
    below = lax.ppermute(own, axis, RIGHT)
    above = lax.ppermute(own, axis, LEFT)
    far_a = lax.ppermute(below[..., :half], axis, RIGHT)
    far_b = lax.ppermute(above[..., half:], axis, LEFT)
    blocks = jnp.zeros((RING, *own.shape), own.dtype)
    zeros = (0,) * (own.ndim - 1)
    for step, block, column in (
        (0, own, 0),
        (3, below, 0),
        (1, above, 0),
        (2, far_a, 0),
        (2, far_b, half),
    ):
        blocks = lax.dynamic_update_slice(blocks, block[None], ((here + step) & 3, *zeros, column))
    return blocks


def scatter_ring(blocks, axis):
    here = lax.axis_index(axis)
    half = blocks.shape[-1] // 2

    def block(step):
        return lax.dynamic_index_in_dim(blocks, (here + step) & 3, 0, keepdims=False)

    far = block(2).astype(BF16)
    got_a = lax.ppermute(far[..., :half], axis, RIGHT)
    got_b = lax.ppermute(far[..., half:], axis, LEFT)
    up, down = block(1).astype(F32), block(3).astype(F32)
    up = jnp.concatenate([up[..., :half] + got_a.astype(F32), up[..., half:]], axis=-1)
    down = jnp.concatenate([down[..., :half], down[..., half:] + got_b.astype(F32)], axis=-1)
    from_below = lax.ppermute(up.astype(BF16), axis, RIGHT)
    from_above = lax.ppermute(down.astype(BF16), axis, LEFT)
    return block(0).astype(F32) + from_below.astype(F32) + from_above.astype(F32)


def per_device(hidden, w_down, ids, gates, cotangent):
    groups = lax.axis_size(GRP)
    slots, inner = hidden.shape
    capacity = slots // (N_HALF * groups)
    half_slots = slots // 2
    rows, width = w_down.shape[1:]
    core, half = lax.axis_index(CORE), lax.axis_index(HALF)
    part = inner // 2

    pair = jnp.concatenate([ids.astype(F32), gates], axis=1)
    pair_p = lax.ppermute(pair, HALF, SWAP)
    cot_p = lax.ppermute(cotangent, HALF, SWAP)
    top = ids.shape[1]
    ids_p, gates_p = pair_p[:, :top].astype(jnp.int32), pair_p[:, top:]

    wz = gather_ring(w_down.reshape(rows, width), ZH)

    first = half * groups
    fills, same, slot_gate, mine = slots_of(ids, gates, cotangent, first, groups, capacity)
    sent = (slot_gate * mine).astype(BF16).reshape(groups, capacity, width)
    grads_own = exchange(sent, GRP)

    wy = gather_ring(wz.reshape(N_ZH * rows, width), Y).reshape(part, width)
    w_other = lax.ppermute(wy, CORE, SWAP)

    fills_p, same_p, slot_gate_p, mine_p = slots_of(ids_p, gates_p, cot_p, first, groups, capacity)
    sent_p = (slot_gate_p * mine_p).astype(BF16).reshape(groups, capacity, width)
    sent_p, grads_own = lax.optimization_barrier((sent_p, grads_own))
    grads_par = exchange(sent_p, GRP)

    hid_own = lax.dynamic_slice_in_dim(hidden, half * half_slots, half_slots, 0)
    hid_par = lax.dynamic_slice_in_dim(hidden, (1 - half) * half_slots, half_slots, 0)
    hid_t = jnp.concatenate([hid_own, hid_par], axis=0).T
    hid_t = hid_t.reshape(N_ZH, N_Y, N_CORE, rows, slots).transpose(2, 1, 0, 3, 4)
    hid_t = hid_t.reshape(N_CORE, part, slots)
    hid_self = lax.dynamic_index_in_dim(hid_t, core, 0, keepdims=False)
    hid_other = lax.dynamic_index_in_dim(hid_t, 1 - core, 0, keepdims=False)
    hid_self, hid_other = lax.optimization_barrier((hid_self, hid_other))

    def project(lo, hi):
        out = dot(hid_self[:, lo:hi], wy, ((0,), (0,))) + dot(hid_other[:, lo:hi], w_other, ((0,), (0,)))
        return out.astype(BF16).reshape(groups, capacity, width)

    out_par, grads_par = lax.optimization_barrier((project(half_slots, slots), grads_par))
    back_par = exchange(out_par, GRP)
    out_own, back_par = lax.optimization_barrier((project(0, half_slots), back_par))
    back_own = exchange(out_own, GRP).reshape(half_slots, width)
    back_par = back_par.reshape(half_slots, width)
    mixed_p, gg_p = combine(back_par, fills_p, same_p, slot_gate_p, mine_p)
    mixed_r = lax.ppermute(mixed_p.astype(BF16), HALF, SWAP)
    gg_r = lax.ppermute(gg_p, HALF, SWAP)
    mixed_o, gg_o = combine(back_own, fills, same, slot_gate, mine)
    mixed = (mixed_o + mixed_r.astype(F32)).astype(BF16)
    gate_grads = (gg_o + gg_r).T

    grads = jnp.concatenate(
        [grads_own.reshape(half_slots, width), grads_par.reshape(half_slots, width)], axis=0
    )
    for_other = dot(hid_other, grads, ((1,), (0,))).astype(BF16)
    got = lax.ppermute(for_other, CORE, SWAP)
    kept = dot(hid_self, grads, ((1,), (0,))) + got.astype(F32)
    by_y = scatter_ring(kept.reshape(RING, N_ZH * rows, width), Y)
    sums = scatter_ring(by_y.reshape(RING, rows, width), ZH)
    weight_grads = sums.astype(BF16).reshape(1, rows, width)

    hg_self = dot(wy, grads, ((1,), (1,))).astype(BF16)
    hg_other = dot(w_other, grads, ((1,), (1,))).astype(BF16)
    low = jnp.where(core == 0, hg_self, hg_other)
    high = jnp.where(core == 0, hg_other, hg_self)
    hg = jnp.stack([low, high]).reshape(N_CORE, N_Y, N_ZH, rows, slots)
    hg = hg.transpose(2, 1, 0, 3, 4).reshape(inner, slots).T
    hidden_grads = jnp.where(half == 0, hg, jnp.roll(hg, half_slots, axis=0))
    return mixed, gate_grads, hidden_grads, weight_grads


def solution(mesh):
    groups = mesh.shape["expert"] // N_HALF
    torus = Mesh(mesh.devices.reshape(N_ZH, N_Y, N_CORE, N_HALF, groups), ALL)
    spread = P(ALL, None)
    weights = P((HALF, GRP), DP, None)

    return jax.shard_map(
        per_device,
        mesh=torus,
        in_specs=(spread, weights, spread, spread, spread),
        out_specs=(spread, spread, spread, weights),
        check_vma=False,
    )
```

```python
import jax
import jax.numpy as jnp
from jax import lax
from jax.sharding import Mesh
from jax.sharding import PartitionSpec as P


ZH, Y, CORE, HALF, GRP = "zh", "y", "core", "half", "grp"
DP = (ZH, Y, CORE)
ALL = (ZH, Y, CORE, HALF, GRP)
N_ZH, N_Y, N_CORE, N_HALF = 4, 4, 2, 2
RING = 4
LANES = 128
RIGHT = [(i, (i + 1) % RING) for i in range(RING)]
LEFT = [(i, (i - 1) % RING) for i in range(RING)]
SWAP = [(0, 1), (1, 0)]
F32, BF16 = jnp.float32, jnp.bfloat16


def dot(a, b, dims):
    return lax.dot_general(a, b, (dims, ((), ())), preferred_element_type=F32)


def exchange(rows, axis):
    return lax.all_to_all(rows, axis, split_axis=0, concat_axis=0, tiled=True)


def slots_of(ids, gates, cotangent, first_expert, experts, capacity):
    top, tokens = ids.shape
    line = jnp.arange(N_HALF * experts * capacity, dtype=jnp.int32)[:, None]
    expert = first_expert + line // (N_HALF * capacity)
    order = jnp.arange(tokens, dtype=jnp.int32)
    source = order // (tokens // N_HALF)
    from_source = (line // capacity) % N_HALF == source[None, :]
    same = [(expert == ids[k][None, :]) & from_source for k in range(top)]
    named = same[0]
    gate = jnp.where(same[0], gates[0][None, :], 0.0)
    for k in range(1, top):
        named = named | same[k]
        gate = jnp.where(same[k], gates[k][None, :], gate)
    before = (order[:, None] < order[None, :]).astype(BF16)
    earlier = dot(named.astype(BF16), before, ((1,), (0,)))
    fills = named & (earlier == (line % capacity).astype(F32))
    slot_gate = jnp.sum(jnp.where(fills, gate, 0.0), axis=1, keepdims=True)
    rows = dot(fills.astype(BF16), cotangent, ((1,), (0,)))
    return fills, same, slot_gate, rows


def combine(returned, fills, same, slot_gate, rows):
    weight = jnp.where(fills, slot_gate, 0.0)
    high = lax.reduce_precision(weight, 8, 7)
    low = (weight - high).astype(BF16)
    mixed = dot(high.astype(BF16), returned, ((0,), (0,))) + dot(low, returned, ((0,), (0,)))
    inner = jnp.sum(returned.astype(F32) * rows.astype(F32), axis=1, keepdims=True)
    spread = jnp.where(fills, inner, 0.0)
    grads = jnp.stack([jnp.sum(jnp.where(s, spread, 0.0), axis=0) for s in same], axis=0)
    return mixed, grads


def pieces_of(value, count):
    found = []
    for _ in range(count):
        piece = lax.reduce_precision(value, 8, 7)
        found.append(piece.astype(BF16))
        value = value - piece
    return found


def beside(rows, columns):
    extra = jnp.concatenate(columns, axis=0).T
    extra = jnp.pad(extra, ((0, 0), (0, LANES - extra.shape[1])))
    return jnp.concatenate([rows, extra], axis=1)


def scatter_ring(blocks, dim, axis):
    here = lax.axis_index(axis)

    def block(step):
        return lax.dynamic_index_in_dim(blocks, (here + step) & 3, dim, keepdims=False)

    far = block(2).astype(BF16)
    cut = 0 if far.ndim == 3 else 1
    half = far.shape[cut] // 2
    low, high = (lambda v: lax.slice_in_dim(v, 0, half, axis=cut)), (
        lambda v: lax.slice_in_dim(v, half, 2 * half, axis=cut)
    )
    got_a = lax.ppermute(low(far), axis, RIGHT)
    got_b = lax.ppermute(high(far), axis, LEFT)
    up, down = block(1).astype(F32), block(3).astype(F32)
    up = jnp.concatenate([low(up) + got_a.astype(F32), high(up)], axis=cut)
    down = jnp.concatenate([low(down), high(down) + got_b.astype(F32)], axis=cut)
    from_below = lax.ppermute(up.astype(BF16), axis, RIGHT)
    from_above = lax.ppermute(down.astype(BF16), axis, LEFT)
    return block(0).astype(F32) + from_below.astype(F32) + from_above.astype(F32)


def gather(value, axis):
    return lax.all_gather(value, axis, axis=0, tiled=True)


def per_device(hidden, w_down, ids, gates, cotangent):
    groups = lax.axis_size(GRP)
    slots, inner = hidden.shape
    capacity = slots // (N_HALF * groups)
    tokens, top = ids.shape
    rows, width = w_down.shape[1:]
    core, half = lax.axis_index(CORE), lax.axis_index(HALF)
    piece = RING // 2 * RING * rows
    part = 2 * piece

    columns = [ids.T.astype(BF16), *pieces_of(gates.T, 3)]
    sent_on = lax.ppermute(beside(cotangent, columns), HALF, SWAP)

    wz = gather(w_down.reshape(rows, width), ZH).reshape(2, piece // RING, width)
    w_self = [gather(wz[i], Y) for i in range(2)]
    w_other = [lax.ppermute(w_self[i], CORE, SWAP) for i in range(2)]

    extra = sent_on[:, width : width + 4 * top].astype(F32).T
    ids_both = jnp.concatenate([ids.T, extra[:top].astype(jnp.int32)], axis=1)
    gates_p = extra[top : 2 * top] + extra[2 * top : 3 * top] + extra[3 * top : 4 * top]
    gates_both = jnp.concatenate([gates.T, gates_p], axis=1)
    cot_both = jnp.concatenate([cotangent, sent_on[:, :width]], axis=0)
    fills, same, slot_gate, picked = slots_of(
        ids_both, gates_both, cot_both, half * groups, groups, capacity
    )
    picked = picked.astype(BF16)
    sent = (slot_gate * picked.astype(F32)).astype(BF16).reshape(groups, N_HALF * capacity, width)
    grads = exchange(sent, GRP).reshape(slots, width)

    hid = hidden.reshape(N_HALF, groups, capacity, inner)
    hid = jnp.where(half == 0, hid, hid[::-1]).transpose(1, 0, 2, 3).reshape(slots, inner)
    hid_t = hid.T.reshape(2, 2, RING, N_CORE, rows, slots).transpose(3, 0, 2, 1, 4, 5)
    hid_t = hid_t.reshape(N_CORE, part, slots)
    hid_self = lax.dynamic_index_in_dim(hid_t, core, 0, keepdims=False)
    hid_other = lax.dynamic_index_in_dim(hid_t, 1 - core, 0, keepdims=False)
    hid_self, hid_other, sent_on = lax.optimization_barrier((hid_self, hid_other, sent_on))

    for_other = dot(hid_other, grads, ((1,), (0,))).astype(BF16)
    got = lax.ppermute(for_other, CORE, SWAP)
    kept = dot(hid_self, grads, ((1,), (0,))) + got.astype(F32)
    kept = kept.reshape(2, RING, piece // RING, width)
    by_y = scatter_ring(kept, 1, Y)
    sums = scatter_ring(by_y.reshape(RING, rows, width), 0, ZH)
    weight_grads = sums.astype(BF16).reshape(1, rows, width)

    out = sum(
        dot(h[i * piece : (i + 1) * piece], w[i], ((0,), (0,)))
        for h, w in ((hid_self, w_self), (hid_other, w_other))
        for i in range(2)
    )
    out = out.astype(BF16).reshape(groups, N_HALF * capacity, width)
    out, grads = lax.optimization_barrier((out, grads))
    back = exchange(out, GRP).reshape(slots, width)
    mixed, gate_grads = combine(back, fills, same, slot_gate, picked)
    passed = beside(mixed[tokens:].astype(BF16), pieces_of(gate_grads[:, tokens:], 2))
    passed = lax.ppermute(passed, HALF, SWAP)
    mixed = (mixed[:tokens] + passed[:, :width].astype(F32)).astype(BF16)
    extra = passed[:, width : width + 2 * top].astype(F32)
    gate_grads = gate_grads[:, :tokens].T + extra[:, :top] + extra[:, top:]

    hg_self, hg_other = (
        jnp.concatenate([dot(w[i], grads, ((1,), (1,))).astype(BF16) for i in range(2)], axis=0)
        for w in (w_self, w_other)
    )
    low = jnp.where(core == 0, hg_self, hg_other)
    high = jnp.where(core == 0, hg_other, hg_self)
    hg = jnp.stack([low, high]).reshape(N_CORE, 2, RING, 2, rows, slots)
    hg = hg.transpose(1, 3, 2, 0, 4, 5).reshape(inner, slots).T
    hg = hg.reshape(groups, N_HALF, capacity, inner).transpose(1, 0, 2, 3)
    hidden_grads = jnp.where(half == 0, hg, hg[::-1]).reshape(slots, inner)
    return mixed, gate_grads, hidden_grads, weight_grads


def solution(mesh):
    groups = mesh.shape["expert"] // N_HALF
    torus = Mesh(mesh.devices.reshape(N_ZH, N_Y, N_CORE, N_HALF, groups), ALL)
    spread = P(ALL, None)
    weights = P((HALF, GRP), DP, None)

    return jax.shard_map(
        per_device,
        mesh=torus,
        in_specs=(spread, weights, spread, spread, spread),
        out_specs=(spread, spread, spread, weights),
        check_vma=False,
    )
```

```python
import jax
import jax.numpy as jnp
from jax import lax
from jax.sharding import Mesh
from jax.sharding import PartitionSpec as P


ZH, Y, CORE, HALF, GRP = "zh", "y", "core", "half", "grp"
DP = (ZH, Y, CORE)
ALL = (ZH, Y, CORE, HALF, GRP)
N_ZH, N_Y, N_CORE, N_HALF = 4, 4, 2, 2
RING = 4
LANES = 128
SWAP = [(0, 1), (1, 0)]
F32, BF16 = jnp.float32, jnp.bfloat16


def dot(a, b, dims):
    return lax.dot_general(a, b, (dims, ((), ())), preferred_element_type=F32)


def exchange(rows, axis):
    return lax.all_to_all(rows, axis, split_axis=0, concat_axis=0, tiled=True)


def slots_of(ids, gates, cotangent, first_expert, experts, capacity):
    top, tokens = ids.shape
    line = jnp.arange(N_HALF * experts * capacity, dtype=jnp.int32)[:, None]
    expert = first_expert + line // (N_HALF * capacity)
    order = jnp.arange(tokens, dtype=jnp.int32)
    source = order // (tokens // N_HALF)
    from_source = (line // capacity) % N_HALF == source[None, :]
    same = [(expert == ids[k][None, :]) & from_source for k in range(top)]
    named = same[0]
    gate = jnp.where(same[0], gates[0][None, :], 0.0)
    for k in range(1, top):
        named = named | same[k]
        gate = jnp.where(same[k], gates[k][None, :], gate)
    before = (order[:, None] < order[None, :]).astype(BF16)
    earlier = dot(named.astype(BF16), before, ((1,), (0,)))
    fills = named & (earlier == (line % capacity).astype(F32))
    slot_gate = jnp.sum(jnp.where(fills, gate, 0.0), axis=1, keepdims=True)
    rows = dot(fills.astype(BF16), cotangent, ((1,), (0,)))
    return fills, same, slot_gate, rows


def combine(returned, fills, same, slot_gate, rows):
    weight = jnp.where(fills, slot_gate, 0.0)
    high = lax.reduce_precision(weight, 8, 7)
    low = (weight - high).astype(BF16)
    mixed = dot(high.astype(BF16), returned, ((0,), (0,))) + dot(low, returned, ((0,), (0,)))
    inner = jnp.sum(returned.astype(F32) * rows.astype(F32), axis=1, keepdims=True)
    spread = jnp.where(fills, inner, 0.0)
    grads = jnp.stack([jnp.sum(jnp.where(s, spread, 0.0), axis=0) for s in same], axis=0)
    return mixed, grads


def pieces_of(value, count):
    found = []
    for _ in range(count):
        piece = lax.reduce_precision(value, 8, 7)
        found.append(piece.astype(BF16))
        value = value - piece
    return found


def beside(rows, columns):
    extra = jnp.concatenate(columns, axis=0).T
    extra = jnp.pad(extra, ((0, 0), (0, LANES - extra.shape[1])))
    return jnp.concatenate([rows, extra], axis=1)


def scatter(blocks, axis):
    here = lax.axis_index(axis)

    def block(step):
        return lax.dynamic_index_in_dim(blocks, (here + step) & 3, 0, keepdims=False)

    total = block(0).astype(F32)
    for step in (2, 1, 3):
        perm = [(i, (i + step) % RING) for i in range(RING)]
        total = total + lax.ppermute(block(step).astype(BF16), axis, perm).astype(F32)
    return total


def gather(value, axis):
    return lax.all_gather(value, axis, axis=0, tiled=True)


def per_device(hidden, w_down, ids, gates, cotangent):
    groups = lax.axis_size(GRP)
    slots, inner = hidden.shape
    capacity = slots // (N_HALF * groups)
    tokens, top = ids.shape
    rows, width = w_down.shape[1:]
    core, half = lax.axis_index(CORE), lax.axis_index(HALF)
    part = RING * RING * rows

    columns = [ids.T.astype(BF16), *pieces_of(gates.T, 3)]
    to_send, weight_rows = lax.optimization_barrier(
        (beside(cotangent, columns), w_down.reshape(rows, width))
    )

    wz = gather(weight_rows, ZH)
    sent_on = lax.ppermute(to_send, HALF, SWAP)
    w_self = exchange(jnp.broadcast_to(wz[None], (RING, *wz.shape)), Y).reshape(part, width)
    w_other = lax.ppermute(w_self, CORE, SWAP)

    extra = sent_on[:, width : width + 4 * top].astype(F32).T
    ids_both = jnp.concatenate([ids.T, extra[:top].astype(jnp.int32)], axis=1)
    gates_p = extra[top : 2 * top] + extra[2 * top : 3 * top] + extra[3 * top : 4 * top]
    gates_both = jnp.concatenate([gates.T, gates_p], axis=1)
    cot_both = jnp.concatenate([cotangent, sent_on[:, :width]], axis=0)
    fills, same, slot_gate, picked = slots_of(
        ids_both, gates_both, cot_both, half * groups, groups, capacity
    )
    picked = picked.astype(BF16)
    sent = (slot_gate * picked.astype(F32)).astype(BF16).reshape(groups, N_HALF * capacity, width)
    sent, w_self = lax.optimization_barrier((sent, w_self))
    grads = exchange(sent, GRP).reshape(slots, width)

    hid = hidden.reshape(N_HALF, groups, capacity, inner)
    hid = jnp.where(half == 0, hid, hid[::-1]).transpose(1, 0, 2, 3).reshape(slots, inner)
    hid_t = hid.T.reshape(RING, RING, N_CORE, rows, slots).transpose(2, 1, 0, 3, 4)
    hid_t = hid_t.reshape(N_CORE, part, slots)
    hid_self = lax.dynamic_index_in_dim(hid_t, core, 0, keepdims=False)
    hid_other = lax.dynamic_index_in_dim(hid_t, 1 - core, 0, keepdims=False)
    hid_self, hid_other = lax.optimization_barrier((hid_self, hid_other))

    out = dot(hid_self, w_self, ((0,), (0,))) + dot(hid_other, w_other, ((0,), (0,)))
    out = out.astype(BF16).reshape(groups, N_HALF * capacity, width)
    out, grads = lax.optimization_barrier((out, grads))

    for_other = dot(hid_other, grads, ((1,), (0,))).astype(BF16)
    got = lax.ppermute(for_other, CORE, SWAP)
    kept = dot(hid_self, grads, ((1,), (0,))) + got.astype(F32)
    by_y = scatter(kept.reshape(RING, RING * rows, width), Y)
    weight_grads = scatter(by_y.reshape(RING, rows, width), ZH)
    weight_grads = weight_grads.astype(BF16).reshape(1, rows, width)

    back = exchange(out, GRP).reshape(slots, width)
    mixed, gate_grads = combine(back, fills, same, slot_gate, picked)
    passed = beside(mixed[tokens:].astype(BF16), pieces_of(gate_grads[:, tokens:], 2))
    passed = lax.ppermute(passed, HALF, SWAP)
    mixed = (mixed[:tokens] + passed[:, :width].astype(F32)).astype(BF16)
    extra = passed[:, width : width + 2 * top].astype(F32)
    gate_grads = gate_grads[:, :tokens].T + extra[:, :top] + extra[:, top:]

    hg_self = dot(w_self, grads, ((1,), (1,))).astype(BF16)
    hg_other = dot(w_other, grads, ((1,), (1,))).astype(BF16)
    low = jnp.where(core == 0, hg_self, hg_other)
    high = jnp.where(core == 0, hg_other, hg_self)
    hg = jnp.stack([low, high]).reshape(N_CORE, RING, RING, rows, slots)
    hg = hg.transpose(2, 1, 0, 3, 4).reshape(inner, slots).T
    hg = hg.reshape(groups, N_HALF, capacity, inner).transpose(1, 0, 2, 3)
    hidden_grads = jnp.where(half == 0, hg, hg[::-1]).reshape(slots, inner)
    return mixed, gate_grads, hidden_grads, weight_grads


def solution(mesh):
    groups = mesh.shape["expert"] // N_HALF
    torus = Mesh(mesh.devices.reshape(N_ZH, N_Y, N_CORE, N_HALF, groups), ALL)
    spread = P(ALL, None)
    weights = P((HALF, GRP), DP, None)

    return jax.shard_map(
        per_device,
        mesh=torus,
        in_specs=(spread, weights, spread, spread, spread),
        out_specs=(spread, spread, spread, weights),
        check_vma=False,
    )
```

```python
import jax
import jax.numpy as jnp
from jax import lax
from jax.sharding import Mesh
from jax.sharding import PartitionSpec as P


ZH, Y, CORE, HALF, GRP = "zh", "y", "core", "half", "grp"
DP = (ZH, Y, CORE)
ALL = (ZH, Y, CORE, HALF, GRP)
N_ZH, N_Y, N_CORE, N_HALF = 4, 4, 2, 2
RING = 4
LANES = 128
SWAP = [(0, 1), (1, 0)]
F32, BF16 = jnp.float32, jnp.bfloat16


def dot(a, b, dims):
    return lax.dot_general(a, b, (dims, ((), ())), preferred_element_type=F32)


def exchange(rows, axis):
    return lax.all_to_all(rows, axis, split_axis=0, concat_axis=0, tiled=True)


def slots_of(ids, gates, cotangent, first_expert, experts, capacity):
    top, tokens = ids.shape
    line = jnp.arange(N_HALF * experts * capacity, dtype=jnp.int32)[:, None]
    expert = first_expert + line // (N_HALF * capacity)
    order = jnp.arange(tokens, dtype=jnp.int32)
    source = order // (tokens // N_HALF)
    from_source = (line // capacity) % N_HALF == source[None, :]
    same = [(expert == ids[k][None, :]) & from_source for k in range(top)]
    named = same[0]
    gate = jnp.where(same[0], gates[0][None, :], 0.0)
    for k in range(1, top):
        named = named | same[k]
        gate = jnp.where(same[k], gates[k][None, :], gate)
    before = (order[:, None] < order[None, :]).astype(BF16)
    earlier = dot(named.astype(BF16), before, ((1,), (0,)))
    fills = named & (earlier == (line % capacity).astype(F32))
    slot_gate = jnp.sum(jnp.where(fills, gate, 0.0), axis=1, keepdims=True)
    rows = dot(fills.astype(BF16), cotangent, ((1,), (0,)))
    return fills, same, slot_gate, rows


def combine(returned, fills, same, slot_gate, rows):
    weight = jnp.where(fills, slot_gate, 0.0)
    high = lax.reduce_precision(weight, 8, 7)
    low = (weight - high).astype(BF16)
    mixed = dot(high.astype(BF16), returned, ((0,), (0,))) + dot(low, returned, ((0,), (0,)))
    inner = jnp.sum(returned.astype(F32) * rows.astype(F32), axis=1, keepdims=True)
    spread = jnp.where(fills, inner, 0.0)
    grads = jnp.stack([jnp.sum(jnp.where(s, spread, 0.0), axis=0) for s in same], axis=0)
    return mixed, grads


def pieces_of(value, count):
    found = []
    for _ in range(count):
        piece = lax.reduce_precision(value, 8, 7)
        found.append(piece.astype(BF16))
        value = value - piece
    return found


def beside(rows, columns):
    extra = jnp.concatenate(columns, axis=0).T
    extra = jnp.pad(extra, ((0, 0), (0, LANES - extra.shape[1])))
    return jnp.concatenate([rows, extra], axis=1)


def forward(step):
    return [(i, (i + step) % RING) for i in range(RING)]


def gather(own, axis):
    got = {4 - step: lax.ppermute(own, axis, forward(step)) for step in (2, 1, 3)}
    return jnp.concatenate([own, got[1], got[2], got[3]], axis=0)


def scatter(blocks, axis):
    total = blocks[0].astype(F32)
    for step in (2, 1, 3):
        got = lax.ppermute(blocks[step].astype(BF16), axis, forward(step))
        total = total + got.astype(F32)
    return total


def turned(blocks, dim, start):
    twice = jnp.concatenate([blocks, blocks], axis=dim)
    return lax.dynamic_slice_in_dim(twice, start, RING, dim)


def per_device(hidden, w_down, ids, gates, cotangent):
    groups = lax.axis_size(GRP)
    slots, inner = hidden.shape
    capacity = slots // (N_HALF * groups)
    tokens, top = ids.shape
    rows, width = w_down.shape[1:]
    core, half = lax.axis_index(CORE), lax.axis_index(HALF)
    zh, y = lax.axis_index(ZH), lax.axis_index(Y)
    part = RING * RING * rows

    columns = [ids.T.astype(BF16), *pieces_of(gates.T, 3)]
    sent_on = lax.ppermute(beside(cotangent, columns), HALF, SWAP)

    w_self = gather(gather(w_down.reshape(rows, width), ZH), Y)
    w_other = lax.ppermute(w_self, CORE, SWAP)

    extra = sent_on[:, width : width + 4 * top].astype(F32).T
    ids_both = jnp.concatenate([ids.T, extra[:top].astype(jnp.int32)], axis=1)
    gates_p = extra[top : 2 * top] + extra[2 * top : 3 * top] + extra[3 * top : 4 * top]
    gates_both = jnp.concatenate([gates.T, gates_p], axis=1)
    cot_both = jnp.concatenate([cotangent, sent_on[:, :width]], axis=0)
    fills, same, slot_gate, picked = slots_of(
        ids_both, gates_both, cot_both, half * groups, groups, capacity
    )
    picked = picked.astype(BF16)
    sent = (slot_gate * picked.astype(F32)).astype(BF16).reshape(groups, N_HALF * capacity, width)
    grads = exchange(sent, GRP).reshape(slots, width)

    hid = hidden.reshape(N_HALF, groups, capacity, inner)
    hid = jnp.where(half == 0, hid, hid[::-1]).transpose(1, 0, 2, 3).reshape(slots, inner)
    hid_t = hid.T.reshape(RING, RING, N_CORE, rows, slots).transpose(2, 1, 0, 3, 4)
    hid_t = turned(turned(hid_t, 2, zh), 1, y)
    hid_t = hid_t.reshape(N_CORE, part, slots)
    hid_self = lax.dynamic_index_in_dim(hid_t, core, 0, keepdims=False)
    hid_other = lax.dynamic_index_in_dim(hid_t, 1 - core, 0, keepdims=False)
    hid_self, hid_other = lax.optimization_barrier((hid_self, hid_other))

    for_other = dot(hid_other, grads, ((1,), (0,))).astype(BF16)
    got = lax.ppermute(for_other, CORE, SWAP)
    kept = dot(hid_self, grads, ((1,), (0,))) + got.astype(F32)
    by_y = scatter(kept.reshape(RING, RING * rows, width), Y)
    weight_grads = scatter(by_y.reshape(RING, rows, width), ZH)
    weight_grads = weight_grads.astype(BF16).reshape(1, rows, width)

    out = dot(hid_self, w_self, ((0,), (0,))) + dot(hid_other, w_other, ((0,), (0,)))
    out = out.astype(BF16).reshape(groups, N_HALF * capacity, width)
    out, grads = lax.optimization_barrier((out, grads))
    back = exchange(out, GRP).reshape(slots, width)
    mixed, gate_grads = combine(back, fills, same, slot_gate, picked)
    passed = beside(mixed[tokens:].astype(BF16), pieces_of(gate_grads[:, tokens:], 2))
    passed = lax.ppermute(passed, HALF, SWAP)
    mixed = (mixed[:tokens] + passed[:, :width].astype(F32)).astype(BF16)
    extra = passed[:, width : width + 2 * top].astype(F32)
    gate_grads = gate_grads[:, :tokens].T + extra[:, :top] + extra[:, top:]

    hg_self = dot(w_self, grads, ((1,), (1,))).astype(BF16)
    hg_other = dot(w_other, grads, ((1,), (1,))).astype(BF16)
    low = jnp.where(core == 0, hg_self, hg_other)
    high = jnp.where(core == 0, hg_other, hg_self)
    hg = jnp.stack([low, high]).reshape(N_CORE, RING, RING, rows, slots)
    hg = turned(turned(hg, 2, (RING - zh) % RING), 1, (RING - y) % RING)
    hg = hg.transpose(2, 1, 0, 3, 4).reshape(inner, slots).T
    hg = hg.reshape(groups, N_HALF, capacity, inner).transpose(1, 0, 2, 3)
    hidden_grads = jnp.where(half == 0, hg, hg[::-1]).reshape(slots, inner)
    return mixed, gate_grads, hidden_grads, weight_grads


def solution(mesh):
    groups = mesh.shape["expert"] // N_HALF
    torus = Mesh(mesh.devices.reshape(N_ZH, N_Y, N_CORE, N_HALF, groups), ALL)
    spread = P(ALL, None)
    weights = P((HALF, GRP), DP, None)

    return jax.shard_map(
        per_device,
        mesh=torus,
        in_specs=(spread, weights, spread, spread, spread),
        out_specs=(spread, spread, spread, weights),
        check_vma=False,
    )
```

```python
import jax
import jax.numpy as jnp
from jax import lax
from jax.sharding import Mesh
from jax.sharding import PartitionSpec as P


ZH, Y, CORE, HALF, GRP = "zh", "y", "core", "half", "grp"
DP = (ZH, Y, CORE)
ALL = (ZH, Y, CORE, HALF, GRP)
N_ZH, N_Y, N_CORE, N_HALF = 4, 4, 2, 2
RING = 4
LANES = 128
SWAP = [(0, 1), (1, 0)]
F32, BF16 = jnp.float32, jnp.bfloat16


def dot(a, b, dims):
    return lax.dot_general(a, b, (dims, ((), ())), preferred_element_type=F32)


def exchange(rows, axis):
    return lax.all_to_all(rows, axis, split_axis=0, concat_axis=0, tiled=True)


def slots_of(ids, gates, cotangent, first_expert, experts, capacity):
    top, tokens = ids.shape
    line = jnp.arange(N_HALF * experts * capacity, dtype=jnp.int32)[:, None]
    expert = first_expert + line // (N_HALF * capacity)
    order = jnp.arange(tokens, dtype=jnp.int32)
    source = order // (tokens // N_HALF)
    from_source = (line // capacity) % N_HALF == source[None, :]
    same = [(expert == ids[k][None, :]) & from_source for k in range(top)]
    named = same[0]
    gate = jnp.where(same[0], gates[0][None, :], 0.0)
    for k in range(1, top):
        named = named | same[k]
        gate = jnp.where(same[k], gates[k][None, :], gate)
    before = (order[:, None] < order[None, :]).astype(BF16)
    earlier = dot(named.astype(BF16), before, ((1,), (0,)))
    fills = named & (earlier == (line % capacity).astype(F32))
    slot_gate = jnp.sum(jnp.where(fills, gate, 0.0), axis=1, keepdims=True)
    rows = dot(fills.astype(BF16), cotangent, ((1,), (0,)))
    return fills, same, slot_gate, rows


def combine(returned, fills, same, slot_gate, rows):
    weight = jnp.where(fills, slot_gate, 0.0)
    high = lax.reduce_precision(weight, 8, 7)
    low = (weight - high).astype(BF16)
    mixed = dot(high.astype(BF16), returned, ((0,), (0,))) + dot(low, returned, ((0,), (0,)))
    inner = jnp.sum(returned.astype(F32) * rows.astype(F32), axis=1, keepdims=True)
    spread = jnp.where(fills, inner, 0.0)
    grads = jnp.stack([jnp.sum(jnp.where(s, spread, 0.0), axis=0) for s in same], axis=0)
    return mixed, grads


def pieces_of(value, count):
    found = []
    for _ in range(count):
        piece = lax.reduce_precision(value, 8, 7)
        found.append(piece.astype(BF16))
        value = value - piece
    return found


def beside(rows, columns):
    extra = jnp.concatenate(columns, axis=0).T
    extra = jnp.pad(extra, ((0, 0), (0, LANES - extra.shape[1])))
    return jnp.concatenate([rows, extra], axis=1)


def forward(step):
    return [(i, (i + step) % RING) for i in range(RING)]


def gather(own, axis):
    got = {4 - step: lax.ppermute(own, axis, forward(step)) for step in (2, 1, 3)}
    return [own, got[1], got[2], got[3]]


def scatter(blocks, axis):
    return [blocks[0]] + [
        lax.ppermute(blocks[step].astype(BF16), axis, forward(step)) for step in (2, 1, 3)
    ]


def total(parts):
    return sum((p.astype(F32) for p in parts[1:]), parts[0].astype(F32))


def turned(blocks, dim, start):
    twice = jnp.concatenate([blocks, blocks], axis=dim)
    return lax.dynamic_slice_in_dim(twice, start, RING, dim)


def per_device(hidden, w_down, ids, gates, cotangent):
    groups = lax.axis_size(GRP)
    slots, inner = hidden.shape
    capacity = slots // (N_HALF * groups)
    tokens, top = ids.shape
    rows, width = w_down.shape[1:]
    core, half = lax.axis_index(CORE), lax.axis_index(HALF)
    zh, y = lax.axis_index(ZH), lax.axis_index(Y)
    part = RING * RING * rows

    columns = [ids.T.astype(BF16), *pieces_of(gates.T, 3)]
    sent_on = lax.ppermute(beside(cotangent, columns), HALF, SWAP)

    wz = jnp.concatenate(gather(w_down.reshape(rows, width), ZH), axis=0)
    wy = gather(wz, Y)

    extra = sent_on[:, width : width + 4 * top].astype(F32).T
    ids_both = jnp.concatenate([ids.T, extra[:top].astype(jnp.int32)], axis=1)
    gates_p = extra[top : 2 * top] + extra[2 * top : 3 * top] + extra[3 * top : 4 * top]
    gates_both = jnp.concatenate([gates.T, gates_p], axis=1)
    cot_both = jnp.concatenate([cotangent, sent_on[:, :width]], axis=0)
    fills, same, slot_gate, picked = slots_of(
        ids_both, gates_both, cot_both, half * groups, groups, capacity
    )
    picked = picked.astype(BF16)
    sent = (slot_gate * picked.astype(F32)).astype(BF16).reshape(groups, N_HALF * capacity, width)
    grads = exchange(sent, GRP).reshape(slots, width)

    hid = hidden.reshape(N_HALF, groups, capacity, inner)
    hid = jnp.where(half == 0, hid, hid[::-1]).transpose(1, 0, 2, 3).reshape(slots, inner)
    hid_t = hid.T.reshape(RING, RING, N_CORE, rows, slots).transpose(2, 1, 0, 3, 4)
    hid_t = turned(turned(hid_t, 2, zh), 1, y)
    hid_t = hid_t.reshape(N_CORE, part, slots)
    hid_self = lax.dynamic_index_in_dim(hid_t, core, 0, keepdims=False)
    hid_other = lax.dynamic_index_in_dim(hid_t, 1 - core, 0, keepdims=False)
    hid_self, hid_other = lax.optimization_barrier((hid_self, hid_other))

    for_other = dot(hid_other, grads, ((1,), (0,))).astype(BF16)
    got = lax.ppermute(for_other, CORE, SWAP)
    kept = dot(hid_self, grads, ((1,), (0,))) + got.astype(F32)
    by_y = total(scatter(kept.reshape(RING, RING * rows, width), Y))
    by_z = scatter(by_y.reshape(RING, rows, width), ZH)

    wy, kept = lax.optimization_barrier((wy, kept))
    w_self = jnp.concatenate(wy, axis=0)
    w_other = lax.ppermute(w_self, CORE, SWAP)
    out = dot(hid_self, w_self, ((0,), (0,))) + dot(hid_other, w_other, ((0,), (0,)))
    out = out.astype(BF16).reshape(groups, N_HALF * capacity, width)
    out, grads = lax.optimization_barrier((out, grads))
    back = exchange(out, GRP).reshape(slots, width)
    mixed, gate_grads = combine(back, fills, same, slot_gate, picked)
    passed = beside(mixed[tokens:].astype(BF16), pieces_of(gate_grads[:, tokens:], 2))
    passed, by_z[0] = lax.optimization_barrier((passed, by_z[0]))
    passed = lax.ppermute(passed, HALF, SWAP)
    weight_grads = total(by_z).astype(BF16).reshape(1, rows, width)
    mixed = (mixed[:tokens] + passed[:, :width].astype(F32)).astype(BF16)
    extra = passed[:, width : width + 2 * top].astype(F32)
    gate_grads = gate_grads[:, :tokens].T + extra[:, :top] + extra[:, top:]

    hg_self = dot(w_self, grads, ((1,), (1,))).astype(BF16)
    hg_other = dot(w_other, grads, ((1,), (1,))).astype(BF16)
    low = jnp.where(core == 0, hg_self, hg_other)
    high = jnp.where(core == 0, hg_other, hg_self)
    hg = jnp.stack([low, high]).reshape(N_CORE, RING, RING, rows, slots)
    hg = turned(turned(hg, 2, (RING - zh) % RING), 1, (RING - y) % RING)
    hg = hg.transpose(2, 1, 0, 3, 4).reshape(inner, slots).T
    hg = hg.reshape(groups, N_HALF, capacity, inner).transpose(1, 0, 2, 3)
    hidden_grads = jnp.where(half == 0, hg, hg[::-1]).reshape(slots, inner)
    return mixed, gate_grads, hidden_grads, weight_grads


def solution(mesh):
    groups = mesh.shape["expert"] // N_HALF
    torus = Mesh(mesh.devices.reshape(N_ZH, N_Y, N_CORE, N_HALF, groups), ALL)
    spread = P(ALL, None)
    weights = P((HALF, GRP), DP, None)

    return jax.shard_map(
        per_device,
        mesh=torus,
        in_specs=(spread, weights, spread, spread, spread),
        out_specs=(spread, spread, spread, weights),
        check_vma=False,
    )
```

```python
import jax
import jax.numpy as jnp
from jax import lax
from jax.sharding import Mesh
from jax.sharding import PartitionSpec as P


ZH, Y, CORE, HALF, GRP = "zh", "y", "core", "half", "grp"
DP = (ZH, Y, CORE)
ALL = (ZH, Y, CORE, HALF, GRP)
N_ZH, N_Y, N_CORE, N_HALF = 4, 4, 2, 2
RING = 4
LANES = 128
SWAP = [(0, 1), (1, 0)]
F32, BF16 = jnp.float32, jnp.bfloat16


def dot(a, b, dims):
    return lax.dot_general(a, b, (dims, ((), ())), preferred_element_type=F32)


def exchange(rows, axis):
    return lax.all_to_all(rows, axis, split_axis=0, concat_axis=0, tiled=True)


def slots_of(ids, gates, cotangent, first_expert, experts, capacity):
    top, tokens = ids.shape
    line = jnp.arange(N_HALF * experts * capacity, dtype=jnp.int32)[:, None]
    expert = first_expert + line // (N_HALF * capacity)
    order = jnp.arange(tokens, dtype=jnp.int32)
    source = order // (tokens // N_HALF)
    from_source = (line // capacity) % N_HALF == source[None, :]
    same = [(expert == ids[k][None, :]) & from_source for k in range(top)]
    named = same[0]
    gate = jnp.where(same[0], gates[0][None, :], 0.0)
    for k in range(1, top):
        named = named | same[k]
        gate = jnp.where(same[k], gates[k][None, :], gate)
    before = (order[:, None] < order[None, :]).astype(BF16)
    earlier = dot(named.astype(BF16), before, ((1,), (0,)))
    fills = named & (earlier == (line % capacity).astype(F32))
    slot_gate = jnp.sum(jnp.where(fills, gate, 0.0), axis=1, keepdims=True)
    rows = dot(fills.astype(BF16), cotangent, ((1,), (0,)))
    return fills, same, slot_gate, rows


def combine(returned, fills, same, slot_gate, rows):
    weight = jnp.where(fills, slot_gate, 0.0)
    high = lax.reduce_precision(weight, 8, 7)
    low = (weight - high).astype(BF16)
    mixed = dot(high.astype(BF16), returned, ((0,), (0,))) + dot(low, returned, ((0,), (0,)))
    inner = jnp.sum(returned.astype(F32) * rows.astype(F32), axis=1, keepdims=True)
    spread = jnp.where(fills, inner, 0.0)
    grads = jnp.stack([jnp.sum(jnp.where(s, spread, 0.0), axis=0) for s in same], axis=0)
    return mixed, grads


def pieces_of(value, count):
    found = []
    for _ in range(count):
        piece = lax.reduce_precision(value, 8, 7)
        found.append(piece.astype(BF16))
        value = value - piece
    return found


def beside(rows, columns):
    extra = jnp.concatenate(columns, axis=0).T
    extra = jnp.pad(extra, ((0, 0), (0, LANES - extra.shape[1])))
    return jnp.concatenate([rows, extra], axis=1)


def forward(step):
    return [(i, (i + step) % RING) for i in range(RING)]


def gather(own, axis):
    got = {4 - step: lax.ppermute(own, axis, forward(step)) for step in (2, 1, 3)}
    return [own, got[1], got[2], got[3]]


def scatter(blocks, axis):
    return [blocks[0]] + [
        lax.ppermute(blocks[step].astype(BF16), axis, forward(step)) for step in (2, 1, 3)
    ]


def total(parts):
    return sum((p.astype(F32) for p in parts[1:]), parts[0].astype(F32))


def turned(blocks, dim, start):
    twice = jnp.concatenate([blocks, blocks], axis=dim)
    return lax.dynamic_slice_in_dim(twice, start, RING, dim)


def per_device(hidden, w_down, ids, gates, cotangent):
    groups = lax.axis_size(GRP)
    slots, inner = hidden.shape
    capacity = slots // (N_HALF * groups)
    tokens, top = ids.shape
    rows, width = w_down.shape[1:]
    core, half = lax.axis_index(CORE), lax.axis_index(HALF)
    zh, y = lax.axis_index(ZH), lax.axis_index(Y)
    part = RING * RING * rows
    half_slots = slots // 2

    columns = [ids.T.astype(BF16), *pieces_of(gates.T, 3)]
    sent_on = lax.ppermute(beside(cotangent, columns), HALF, SWAP)

    wz = jnp.concatenate(gather(w_down.reshape(rows, width), ZH), axis=0)
    wy = gather(wz, Y)

    extra = sent_on[:, width : width + 4 * top].astype(F32).T
    ids_both = jnp.concatenate([ids.T, extra[:top].astype(jnp.int32)], axis=1)
    gates_p = extra[top : 2 * top] + extra[2 * top : 3 * top] + extra[3 * top : 4 * top]
    gates_both = jnp.concatenate([gates.T, gates_p], axis=1)
    cot_both = jnp.concatenate([cotangent, sent_on[:, :width]], axis=0)
    fills, same, slot_gate, picked = slots_of(
        ids_both, gates_both, cot_both, half * groups, groups, capacity
    )
    picked = picked.astype(BF16)
    sent = (slot_gate * picked.astype(F32)).astype(BF16).reshape(groups, N_HALF * capacity, width)
    grads = exchange(sent, GRP).reshape(slots, width)

    hid = hidden.reshape(N_HALF, half_slots, inner)
    hid = jnp.where(half == 0, hid, hid[::-1])

    def by_place(rows_of):
        cut = rows_of.T.reshape(RING, RING, N_CORE, rows, slots).transpose(2, 1, 0, 3, 4)
        cut = turned(turned(cut, 2, zh), 1, y).reshape(N_CORE, part, slots)
        return tuple(
            lax.dynamic_index_in_dim(cut, c, 0, keepdims=False) for c in (core, 1 - core)
        )

    hid_p = by_place(hid.reshape(slots, inner))
    hid = hid.reshape(N_HALF, groups, capacity, inner).transpose(1, 0, 2, 3)
    hid_self, hid_other = by_place(hid.reshape(slots, inner))

    def share(source):
        def cut(v):
            return v.reshape(groups, N_HALF, capacity, -1)[:, source].reshape(half_slots, -1)

        mine = slice(source * tokens, (source + 1) * tokens)
        return cut(fills)[:, mine], [cut(v)[:, mine] for v in same], cut(slot_gate), cut(picked)

    early = (hid_p, hid_self, hid_other, share(0), share(1))
    hid_p, hid_self, hid_other, share_own, share_par = lax.optimization_barrier(early)

    for_other = dot(hid_other, grads, ((1,), (0,))).astype(BF16)
    got = lax.ppermute(for_other, CORE, SWAP)
    kept = dot(hid_self, grads, ((1,), (0,))) + got.astype(F32)
    by_y = total(scatter(kept.reshape(RING, RING * rows, width), Y))
    by_z = scatter(by_y.reshape(RING, rows, width), ZH)

    w_self = jnp.concatenate(wy, axis=0)
    w_other = lax.ppermute(w_self, CORE, SWAP)

    def project(lo):
        own, other = (h[:, lo : lo + half_slots] for h in hid_p)
        out = dot(own, w_self, ((0,), (0,))) + dot(other, w_other, ((0,), (0,)))
        return out.astype(BF16).reshape(groups, capacity, width)

    out_par, grads = lax.optimization_barrier((project(half_slots), grads))
    back_par = exchange(out_par, GRP)
    out_own, back_par = lax.optimization_barrier((project(0), back_par))
    back_own = exchange(out_own, GRP).reshape(half_slots, width)
    passed, gg = combine(back_par.reshape(half_slots, width), *share_par)
    passed = beside(passed.astype(BF16), pieces_of(gg, 2))
    passed, by_z[0] = lax.optimization_barrier((passed, by_z[0]))
    back_own, _ = lax.optimization_barrier((back_own, passed))
    passed = lax.ppermute(passed, HALF, SWAP)
    mixed, gg = combine(back_own, *share_own)
    passed, mixed, gg = lax.optimization_barrier((passed, mixed, gg))
    mixed = (mixed + passed[:, :width].astype(F32)).astype(BF16)
    extra = passed[:, width : width + 2 * top].astype(F32)
    gate_grads = gg.T + extra[:, :top] + extra[:, top:]
    weight_grads = total(by_z).astype(BF16).reshape(1, rows, width)

    hg_self = dot(w_self, grads, ((1,), (1,))).astype(BF16)
    hg_other = dot(w_other, grads, ((1,), (1,))).astype(BF16)
    low = jnp.where(core == 0, hg_self, hg_other)
    high = jnp.where(core == 0, hg_other, hg_self)
    hg = jnp.stack([low, high]).reshape(N_CORE, RING, RING, rows, slots)
    hg = turned(turned(hg, 2, (RING - zh) % RING), 1, (RING - y) % RING)
    hg = hg.transpose(2, 1, 0, 3, 4).reshape(inner, slots).T
    hg = hg.reshape(groups, N_HALF, capacity, inner).transpose(1, 0, 2, 3)
    hidden_grads = jnp.where(half == 0, hg, hg[::-1]).reshape(slots, inner)
    return mixed, gate_grads, hidden_grads, weight_grads


def solution(mesh):
    groups = mesh.shape["expert"] // N_HALF
    torus = Mesh(mesh.devices.reshape(N_ZH, N_Y, N_CORE, N_HALF, groups), ALL)
    spread = P(ALL, None)
    weights = P((HALF, GRP), DP, None)

    return jax.shard_map(
        per_device,
        mesh=torus,
        in_specs=(spread, weights, spread, spread, spread),
        out_specs=(spread, spread, spread, weights),
        check_vma=False,
    )
```

```python
import jax
import jax.numpy as jnp
from jax import lax
from jax.sharding import Mesh
from jax.sharding import PartitionSpec as P


ZH, Y, CORE, HALF, GRP = "zh", "y", "core", "half", "grp"
DP = (ZH, Y, CORE)
ALL = (ZH, Y, CORE, HALF, GRP)
N_ZH, N_Y, N_CORE, N_HALF = 4, 4, 2, 2
RING = 4
LANES = 128
SWAP = [(0, 1), (1, 0)]
F32, BF16 = jnp.float32, jnp.bfloat16


def dot(a, b, dims):
    return lax.dot_general(a, b, (dims, ((), ())), preferred_element_type=F32)


def exchange(rows, axis):
    return lax.all_to_all(rows, axis, split_axis=0, concat_axis=0, tiled=True)


def slots_of(ids, gates, cotangent, first_expert, experts, capacity):
    top, tokens = ids.shape
    line = jnp.arange(N_HALF * experts * capacity, dtype=jnp.int32)[:, None]
    expert = first_expert + line // (N_HALF * capacity)
    order = jnp.arange(tokens, dtype=jnp.int32)
    source = order // (tokens // N_HALF)
    from_source = (line // capacity) % N_HALF == source[None, :]
    same = [(expert == ids[k][None, :]) & from_source for k in range(top)]
    named = same[0]
    gate = jnp.where(same[0], gates[0][None, :], 0.0)
    for k in range(1, top):
        named = named | same[k]
        gate = jnp.where(same[k], gates[k][None, :], gate)
    before = (order[:, None] < order[None, :]).astype(BF16)
    earlier = dot(named.astype(BF16), before, ((1,), (0,)))
    fills = named & (earlier == (line % capacity).astype(F32))
    slot_gate = jnp.sum(jnp.where(fills, gate, 0.0), axis=1, keepdims=True)
    rows = dot(fills.astype(BF16), cotangent, ((1,), (0,)))
    return fills, same, slot_gate, rows


def combine(returned, fills, same, slot_gate, rows):
    weight = jnp.where(fills, slot_gate, 0.0)
    high = lax.reduce_precision(weight, 8, 7)
    low = (weight - high).astype(BF16)
    mixed = dot(high.astype(BF16), returned, ((0,), (0,))) + dot(low, returned, ((0,), (0,)))
    inner = jnp.sum(returned.astype(F32) * rows.astype(F32), axis=1, keepdims=True)
    spread = jnp.where(fills, inner, 0.0)
    grads = jnp.stack([jnp.sum(jnp.where(s, spread, 0.0), axis=0) for s in same], axis=0)
    return mixed, grads


def pieces_of(value, count):
    found = []
    for _ in range(count):
        piece = lax.reduce_precision(value, 8, 7)
        found.append(piece.astype(BF16))
        value = value - piece
    return found


def beside(rows, columns):
    extra = jnp.concatenate(columns, axis=0).T
    extra = jnp.pad(extra, ((0, 0), (0, LANES - extra.shape[1])))
    return jnp.concatenate([rows, extra], axis=1)


def forward(step):
    return [(i, (i + step) % RING) for i in range(RING)]


def gather(own, axis):
    got = {4 - step: lax.ppermute(own, axis, forward(step)) for step in (2, 1, 3)}
    return [own, got[1], got[2], got[3]]


def scatter(blocks, axis):
    return [blocks[0]] + [
        lax.ppermute(blocks[step].astype(BF16), axis, forward(step)) for step in (2, 1, 3)
    ]


def total(parts):
    return sum((p.astype(F32) for p in parts[1:]), parts[0].astype(F32))


def turned(blocks, dim, start):
    twice = jnp.concatenate([blocks, blocks], axis=dim)
    return lax.dynamic_slice_in_dim(twice, start, RING, dim)


def per_device(hidden, w_down, ids, gates, cotangent):
    groups = lax.axis_size(GRP)
    slots, inner = hidden.shape
    capacity = slots // (N_HALF * groups)
    tokens, top = ids.shape
    rows, width = w_down.shape[1:]
    core, half = lax.axis_index(CORE), lax.axis_index(HALF)
    zh, y = lax.axis_index(ZH), lax.axis_index(Y)
    part = RING * RING * rows

    columns = [ids.T.astype(BF16), *pieces_of(gates.T, 3)]
    sent_on = lax.ppermute(beside(cotangent, columns), HALF, SWAP)

    wz = gather(w_down.reshape(rows, width), ZH)

    hid = hidden.reshape(N_HALF, groups, capacity, inner)
    hid = jnp.where(half == 0, hid, hid[::-1]).transpose(1, 0, 2, 3).reshape(slots, inner)
    hid_t = hid.T.reshape(RING, RING, N_CORE, rows, slots).transpose(2, 1, 0, 3, 4)
    hid_t = turned(turned(hid_t, 2, zh), 1, y)
    hid_t = hid_t.reshape(N_CORE, part, slots)
    hid_self = lax.dynamic_index_in_dim(hid_t, core, 0, keepdims=False)
    hid_other = lax.dynamic_index_in_dim(hid_t, 1 - core, 0, keepdims=False)
    wz, hid_self, hid_other = lax.optimization_barrier((wz, hid_self, hid_other))
    wy = gather(jnp.concatenate(wz, axis=0), Y)

    extra = sent_on[:, width : width + 4 * top].astype(F32).T
    ids_both = jnp.concatenate([ids.T, extra[:top].astype(jnp.int32)], axis=1)
    gates_p = extra[top : 2 * top] + extra[2 * top : 3 * top] + extra[3 * top : 4 * top]
    gates_both = jnp.concatenate([gates.T, gates_p], axis=1)
    cot_both = jnp.concatenate([cotangent, sent_on[:, :width]], axis=0)
    fills, same, slot_gate, picked = slots_of(
        ids_both, gates_both, cot_both, half * groups, groups, capacity
    )
    picked = picked.astype(BF16)
    sent = (slot_gate * picked.astype(F32)).astype(BF16).reshape(groups, N_HALF * capacity, width)
    grads = exchange(sent, GRP).reshape(slots, width)

    for_other = dot(hid_other, grads, ((1,), (0,))).astype(BF16)
    got = lax.ppermute(for_other, CORE, SWAP)
    kept = dot(hid_self, grads, ((1,), (0,))) + got.astype(F32)
    by_y = total(scatter(kept.reshape(RING, RING * rows, width), Y))
    by_z = scatter(by_y.reshape(RING, rows, width), ZH)

    w_self = jnp.concatenate(wy, axis=0)
    w_other = lax.ppermute(w_self, CORE, SWAP)
    w_other, _ = lax.optimization_barrier((w_other, for_other))
    out = dot(hid_self, w_self, ((0,), (0,))) + dot(hid_other, w_other, ((0,), (0,)))
    out = out.astype(BF16).reshape(groups, N_HALF * capacity, width)
    out, grads = lax.optimization_barrier((out, grads))
    back = exchange(out, GRP).reshape(slots, width)
    mixed, gate_grads = combine(back, fills, same, slot_gate, picked)
    passed = beside(mixed[tokens:].astype(BF16), pieces_of(gate_grads[:, tokens:], 2))
    passed, by_z[0] = lax.optimization_barrier((passed, by_z[0]))
    passed = lax.ppermute(passed, HALF, SWAP)
    weight_grads = total(by_z).astype(BF16).reshape(1, rows, width)
    mixed = (mixed[:tokens] + passed[:, :width].astype(F32)).astype(BF16)
    extra = passed[:, width : width + 2 * top].astype(F32)
    gate_grads = gate_grads[:, :tokens].T + extra[:, :top] + extra[:, top:]

    hg_self = dot(w_self, grads, ((1,), (1,))).astype(BF16)
    hg_other = dot(w_other, grads, ((1,), (1,))).astype(BF16)
    low = jnp.where(core == 0, hg_self, hg_other)
    high = jnp.where(core == 0, hg_other, hg_self)
    hg = jnp.stack([low, high]).reshape(N_CORE, RING, RING, rows, slots)
    hg = turned(turned(hg, 2, (RING - zh) % RING), 1, (RING - y) % RING)
    hg = hg.transpose(2, 1, 0, 3, 4).reshape(inner, slots).T
    hg = hg.reshape(groups, N_HALF, capacity, inner).transpose(1, 0, 2, 3)
    hidden_grads = jnp.where(half == 0, hg, hg[::-1]).reshape(slots, inner)
    return mixed, gate_grads, hidden_grads, weight_grads


def solution(mesh):
    groups = mesh.shape["expert"] // N_HALF
    torus = Mesh(mesh.devices.reshape(N_ZH, N_Y, N_CORE, N_HALF, groups), ALL)
    spread = P(ALL, None)
    weights = P((HALF, GRP), DP, None)

    return jax.shard_map(
        per_device,
        mesh=torus,
        in_specs=(spread, weights, spread, spread, spread),
        out_specs=(spread, spread, spread, weights),
        check_vma=False,
    )
```
